32 devices in a mesh: group: 2 (over x), ep: 16 (over z, y, core).
Axes of the slice: x: 2, y: 2, z: 4, core: 2. Of those that a mesh axis runs over, the one named last changes fastest.
Arguments:
- tokens: bfloat16 [2048, 3072], P(('group', 'ep')), parts along dimension 0, may hold values from -6 to 6
- expert_ids: int32 [2048, 2], P(('group', 'ep')), parts along dimension 0, may hold values from 0 to 3, all different within a row; in each aligned block of 64 rows (0 to 63, 64 to 127, ...) at most 48 rows name the same one
- w_router: bfloat16 [3072, 4], replicated, may hold values from -0.109375 to 0.109375
- w_gate: bfloat16 [3072, 32768], P(None, 'ep'), may hold values from -0.109375 to 0.109375
- w_up: bfloat16 [3072, 32768], P(None, 'ep'), may hold values from -0.109375 to 0.109375
- w_down: bfloat16 [32768, 3072], P('ep'), may hold values from -0.0625 to 0.0625
- queries: bfloat16 [256, 24, 128], P(('group', 'ep')), parts along dimension 0, may hold values from -48 to 48
- key_cache: bfloat16 [256, 256, 4, 128], P(('group', 'ep')), parts along dimension 0, may hold values from -48 to 48
- cached_value_rows: bfloat16 [256, 256, 4, 128], P(('group', 'ep')), parts along dimension 0, may hold values from -6 to 6
- lengths: int32 [256], P(('group', 'ep')), parts along dimension 0, may hold values from 2 to 256, as said below
Outputs:
- moe_out: bfloat16 [2048, 3072], P(('group', 'ep')), parts along dimension 0
- attention_out: bfloat16 [256, 24, 128], P(('group', 'ep')), parts along dimension 0
The draws below stay inside these ranges and needn't reach their ends.
There are 2 independent parts, one for each index of `group`. The reference program is written for one: setup_inputs(seed, part) draws one part's arguments, and reference() takes and returns one part's arrays. A program takes and returns all parts, laid end to end along the dimension named above; an argument that names none is the same for every part. Nothing has to cross between parts.
Inputs may be any that keep to these rules, and one draw needn't show every extreme that they name: `expert_ids`: each row names two different experts; among the rows of one device no expert is named more than 48 times, and some device has an expert named exactly 48 times. `lengths`: every device holds a request of length 256.
All inputs are finite; a program needn't handle non-finite values.
Results may differ from the reference program's by a relative error of at most 0.0085.
Values may be sent and summed in bfloat16 or wider, within the bound.
A program may use at most 128 MiB of HBM per device.

```python
import math
import jax
import jax.numpy as jnp
import numpy as np
from jax import lax

D = 3072
E = 4
FF = 8192
HEAD_SIZE = 128
KEY_VALUE_HEADS = 4
HQ = 24
TOK_DEV = 64
DEC_DEV = 8
CACHE_POSITIONS = 256
CAP = 48
TP = 4
FF_DEV = 2048
TOKENS = 1024
DECODE_REQUESTS = 128
N_EP = 16


def attention_draw(key):
    base = jax.random.fold_in(key, 4242)
    query_key, cache_random_seed = jax.random.split(base, 2)
    query_draw = jnp.clip(jax.random.normal(query_key, (DECODE_REQUESTS, HQ, HEAD_SIZE), jnp.float32), -6.0, 6.0)
    cache_sample_seed = jnp.clip(jax.random.normal(cache_random_seed, (DECODE_REQUESTS, CACHE_POSITIONS, KEY_VALUE_HEADS, HEAD_SIZE), jnp.float32), -6.0, 6.0)
    return (query_draw, cache_sample_seed)


def draw_queries(key, part):
    return attention_draw(key)[0].astype(jnp.bfloat16)


def draw_key_cache(key, part):
    return attention_draw(key)[1].astype(jnp.bfloat16)


def draw_lengths(key, part):
    base = jax.random.fold_in(key, 77)
    first_key, second_key = jax.random.split(base)
    devices_here = DECODE_REQUESTS // DEC_DEV
    drawn = jax.random.randint(first_key, (devices_here, DEC_DEV), 2, CACHE_POSITIONS + 1, jnp.int32)
    longest = jax.random.randint(second_key, (devices_here, 1), 0, DEC_DEV, jnp.int32)
    filled = jnp.where(jnp.arange(DEC_DEV, dtype=jnp.int32)[None, :] == longest, CACHE_POSITIONS, drawn)
    return filled.reshape(DECODE_REQUESTS)


def block_levels(rng, extent, shards, low, top_value):
    def one(dim, parts):
        heights = jax.random.uniform(jax.random.fold_in(jax.random.fold_in(rng, 6), dim), (parts,), jnp.float32, low / len(shards), top_value / len(shards))
        return jnp.repeat(jnp.exp(heights), extent[dim] // parts).reshape((-1,) + (1,) * (len(extent) - dim - 1))

    level = one(*shards[0])
    for cut in shards[1:]:
        level = level * one(*cut)
    return level


def shared_out(key, own, number, rows, number_of, top, most, slope):
    order = jax.random.permutation(key, number_of)
    packed, usual = load_shares(number_of, rows * top, most, slope, True), load_shares(number_of, rows * top, most, slope, False)
    places = jnp.arange(number_of)

    def named(tallies, rotation):
        used = int((tallies > 0).sum())
        fixed = max(1, used // 4)
        shifted = fixed + (places - fixed + rotation * (used - fixed)) % max(1, number_of - fixed)
        return jnp.zeros((number_of,), jnp.int32).at[order[jnp.where(places < fixed, places, shifted)]].set(jnp.asarray(tallies, jnp.int32))

    tallies = jnp.where(number % 4 == 0, named(packed, number // 4), named(usual, number - number // 4 - 1))
    mixed = jax.random.permutation(jax.random.fold_in(own, 3), number_of)
    donor, taker = mixed[0:number_of // 2 * 2:2], mixed[1:number_of // 2 * 2:2]
    margin = jnp.minimum(tallies[donor] - 1, most - tallies[taker]) // 2
    margin = jnp.where((donor == order[0]) | (taker == order[0]) | (tallies[taker] == 0), 0, jnp.maximum(margin, 0))
    shifted = jax.random.randint(jax.random.fold_in(own, 4), (number_of // 2,), 0, 1 << 20) % (margin + 1)
    tallies = tallies.at[donor].add(-shifted).at[taker].add(shifted)
    items = jnp.searchsorted(jnp.cumsum(tallies), jnp.arange(rows * top), side="right").astype(jnp.int32)
    grid = items.reshape(top, rows).T
    grid = grid[jax.random.permutation(jax.random.fold_in(own, 1), rows)]
    rotation = jax.random.randint(jax.random.fold_in(own, 2), (rows, 1), 0, top)
    return jnp.take_along_axis(grid, (jnp.arange(top)[None, :] + rotation) % top, axis=1)


def load_shares(number_of, total, reach, lean, full):
    loads = [(1 << 20) // math.isqrt(standing ** lean) + 1 for standing in range(1, number_of + 1)]
    largest = reach if full else min(reach, max(-(-total // number_of), total * loads[0] // sum(loads)))
    least = 1 if total - largest >= number_of - 1 else 0
    holding, spare = [largest] + [least] * (number_of - 1), total - largest - least * (number_of - 1)
    while spare > 0:
        movable = [i for i in range(1, number_of) if holding[i] < largest] or [i for i in range(1, number_of) if holding[i] < reach]
        pool, budget = sum([loads[i] for i in movable]), spare
        for i in movable:
            addition = min(reach - holding[i], max(1, budget * loads[i] // pool), spare)
            holding[i] = holding[i] + addition
            spare = spare - addition
    return np.array(holding)


def centred(stream_key, shape, width, reach, cuts=(), kind=jnp.bfloat16):
    result = jax.random.normal(stream_key, shape, jnp.float32) * width
    if len(cuts) > 0:
        result = block_levels(stream_key, shape, cuts, -0.22, 0.18) * result
    return jnp.clip(result, min=-reach, max=reach).astype(kind)


def setup_inputs(seed: int = 0, part: int = 0) -> dict:
    key_list = jax.random.split(jax.random.key(seed), 11)
    own_keys = jax.random.split(jax.random.fold_in(key_list[10], part), 11)
    tokens = centred(own_keys[0], (TOKENS, D), 1.0, 6.0, ((0, 16),))
    expert_ids_keys = jax.random.split(jax.random.fold_in(own_keys[1], 1), TOKENS // TOK_DEV)
    expert_ids_turns = jax.random.permutation(jax.random.fold_in(own_keys[1], 3), TOKENS // TOK_DEV)
    expert_ids = jax.vmap(lambda own, number: shared_out(jax.random.fold_in(own_keys[1], 2), own, number, TOK_DEV, E, 2, CAP, 2))(expert_ids_keys, expert_ids_turns).reshape((TOKENS, 2))
    w_router = centred(key_list[2], (D, E), D ** -0.5, 0.109375)
    w_gate = centred(key_list[3], (D, E * FF), D ** -0.5, 0.109375, ((1, 16),))
    w_up = centred(key_list[4], (D, E * FF), D ** -0.5, 0.109375, ((1, 16),))
    w_down = centred(key_list[5], (E * FF, D), FF ** -0.5, 0.0625, ((0, 16),))
    queries = draw_queries(jax.random.fold_in(jax.random.fold_in(key_list[10], part), 71), part)
    key_cache = draw_key_cache(jax.random.fold_in(jax.random.fold_in(key_list[10], part), 71), part)
    cached_value_rows = centred(own_keys[8], (DECODE_REQUESTS, CACHE_POSITIONS, KEY_VALUE_HEADS, HEAD_SIZE), 1.0, 6.0, ((0, 16),))
    lengths = draw_lengths(jax.random.fold_in(jax.random.fold_in(key_list[10], part), 71), part)
    return {"tokens": tokens, "expert_ids": expert_ids, "w_router": w_router, "w_gate": w_gate, "w_up": w_up, "w_down": w_down, "queries": queries, "key_cache": key_cache, "cached_value_rows": cached_value_rows, "lengths": lengths}


def expert_mlp(inputs, gate_part, up_part, down_part):
    gate_value = jnp.dot(inputs, gate_part, preferred_element_type=jnp.float32)
    up_value = jnp.dot(inputs, up_part, preferred_element_type=jnp.float32)
    hidden = (jax.nn.silu(gate_value) * up_value).astype(jnp.bfloat16)
    row_count = hidden.shape[0]
    split_hidden = hidden.reshape(row_count, TP, FF_DEV).astype(jnp.float32)
    split_down = down_part.reshape(TP, FF_DEV, D).astype(jnp.float32)
    shares = jnp.einsum("rsf,sfd->rsd", split_hidden, split_down, precision=lax.Precision.HIGHEST).astype(jnp.bfloat16)
    shares = lax.optimization_barrier(shares)
    return jnp.sum(shares.astype(jnp.float32), axis=1)


def route_tables(tokens, expert_ids, w_router, capacity):
    token_count = tokens.shape[0]
    expert_count = w_router.shape[1]
    logits = jnp.dot(tokens, w_router, preferred_element_type=jnp.float32)
    labels = jnp.arange(expert_count, dtype=jnp.int32)
    onehot = expert_ids[:, :, None] == labels[None, None, :]
    picked = jnp.sum(jnp.where(onehot, logits[:, None, :], jnp.float32(0.0)), axis=2)
    gate_values = 1.0 / (1.0 + jnp.exp(picked[:, ::-1] - picked))
    flat_hits = onehot.reshape(token_count * 2, expert_count).astype(jnp.int32)
    earlier = jnp.cumsum(flat_hits, axis=0) - flat_hits
    position = jnp.sum(earlier * flat_hits, axis=1).reshape(token_count, 2)
    return gate_values, expert_ids * capacity + position


def decode_attention(queries, key_cache, cached_value_rows, lengths):
    request_count, head_count, head_dim = queries.shape
    cache_len = key_cache.shape[1]
    kv_heads = key_cache.shape[2]
    grouped = queries.reshape(request_count, kv_heads, head_count // kv_heads, head_dim).astype(jnp.float32)
    scores = jnp.einsum("bkgd,blkd->bkgl", grouped, key_cache.astype(jnp.float32), precision=lax.Precision.HIGHEST) * (head_dim ** -0.5)
    visible = jnp.arange(cache_len, dtype=jnp.int32)[None, :] < lengths[:, None]
    scores = jnp.where(visible[:, None, None, :], scores, -jnp.inf)
    row_max = jnp.max(scores, axis=3, keepdims=True)
    exponent = jnp.exp(scores - row_max)
    weights = (exponent / jnp.sum(exponent, axis=3, keepdims=True)).astype(jnp.bfloat16)
    mixed = jnp.einsum("bkgl,blkd->bkgd", weights.astype(jnp.float32), cached_value_rows.astype(jnp.float32), precision=lax.Precision.HIGHEST)
    return mixed.reshape(request_count, head_count, head_dim).astype(jnp.bfloat16)


def reference(tokens, expert_ids, w_router, w_gate, w_up, w_down, queries, key_cache, cached_value_rows, lengths):
    blocks = tokens.reshape(N_EP, TOK_DEV, D)
    block_ids = expert_ids.reshape(N_EP, TOK_DEV, 2)

    def per_source(block_tokens, block_choice):
        return route_tables(block_tokens, block_choice, w_router, CAP)

    gate_values, slot_index = jax.vmap(per_source)(blocks, block_ids)
    position = slot_index - block_ids * CAP
    source = jnp.arange(N_EP, dtype=jnp.int32)[:, None, None] + jnp.zeros((N_EP, TOK_DEV, 2), jnp.int32)
    buffer_row = source * CAP + position
    token_row = source * TOK_DEV + jnp.arange(TOK_DEV, dtype=jnp.int32)[None, :, None]
    table = jnp.full((E, N_EP * CAP), TOKENS, jnp.int32)
    table = table.at[block_ids.reshape(-1), buffer_row.reshape(-1)].set(token_row.reshape(-1))
    padded = jnp.concatenate([tokens, jnp.zeros((1, D), jnp.bfloat16)], axis=0)
    outputs = []
    for expert in range(E):
        inputs = padded[table[expert]]
        outputs.append(expert_mlp(inputs, w_gate[:, expert * FF:(expert + 1) * FF], w_up[:, expert * FF:(expert + 1) * FF], w_down[expert * FF:(expert + 1) * FF, :]))
    stacked = jnp.stack(outputs)
    picked = stacked[block_ids, buffer_row]
    moe_out = jnp.sum(gate_values[..., None] * picked, axis=2).reshape(TOKENS, D).astype(jnp.bfloat16)
    attention_out = decode_attention(queries, key_cache, cached_value_rows, lengths)
    return moe_out, attention_out
```

```python
import functools

import jax
import jax.numpy as jnp
from jax import lax
from jax.experimental import pallas as pl
from jax.experimental.pallas import tpu as pltpu
from jax.sharding import PartitionSpec as P

CAP = 48
UP_TILE = 512
DOWN_TILE = 1024
CHUNK = 1024
VMEM_LIMIT = 66_000_000
MESH = pl.DeviceIdType.MESH


def flip(index, mask):
    result = index
    bit = 1
    while bit <= mask:
        if mask & bit:
            result = result + bit - 2 * bit * ((index // bit) % 2)
        bit *= 2
    return result


def moe_kernel(
    plane,
    kv_heads,
    tokens,
    ids,
    router,
    queries,
    lengths,
    wg_hbm,
    wu_hbm,
    wd_hbm,
    k_hbm,
    v_hbm,
    out,
    att_out,
    wg,
    wu,
    wd,
    keys,
    values,
    pos,
    gate,
    comb,
    line,
    line_pos,
    outbox,
    arrived,
    hidden,
    partial,
    got_core,
    got_y,
    got_z,
    w_sems,
    d_sems,
    kv_sems,
    send_sems,
    recv_sems,
):
    me = lax.axis_index("ep")
    experts = router.shape[0]
    count, features = tokens.shape
    z = me // plane
    mid = (z % (experts - 1) + 1) // 2
    core_peer = flip(me, 1)
    y_peer = flip(me, 2)
    z_peers = [flip(me, plane * d) for d in range(experts)]
    xors = [0, 2 + mid, 3 - mid, 1]
    homes = [
        me,
        z_peers[2] + mid * (z_peers[3] - z_peers[2]),
        z_peers[3] + mid * (z_peers[2] - z_peers[3]),
        z_peers[1],
    ]
    n_up = wg.shape[0]
    n_down = wd.shape[0]
    up_tile = wg.shape[2]
    down_tile = wd.shape[2]

    def on_end(body):
        pl.when(mid == 0)(body)

    def on_mid(body):
        pl.when(mid == 1)(body)

    def kv_copy(i):
        src, dst = ((k_hbm, keys), (v_hbm, values))[i]
        return pltpu.make_async_copy(src, dst, kv_sems.at[i])

    def up_copy(i, j):
        src, dst = ((wg_hbm, wg), (wu_hbm, wu))[i]
        cols = pl.ds(pl.multiple_of(j * up_tile, up_tile), up_tile)
        return pltpu.make_async_copy(src.at[:, cols], dst.at[j], w_sems.at[i, j])

    def down_copy(j):
        cols = pl.ds(pl.multiple_of(j * down_tile, down_tile), down_tile)
        return pltpu.make_async_copy(wd_hbm.at[:, cols], wd.at[j], d_sems.at[j])

    barrier = pltpu.get_barrier_semaphore()
    peers = [core_peer, y_peer] + z_peers[1:]
    for peer in peers:
        pl.semaphore_signal(barrier, inc=1, device_id={"ep": peer}, device_id_type=MESH)
    kv_copy(0).start()
    kv_copy(1).start()
    up_copy(0, 0).start()
    up_copy(1, 0).start()

    row = lax.broadcasted_iota(jnp.int32, (8, count), 0)
    label = jnp.full((8, count), -1, jnp.int32)
    for d in range(experts):
        label = jnp.where(row == d, flip(z, d), label)
    first_hit = ids[0:1, :] == label
    second_hit = ids[1:2, :] == label
    hit = first_hit | second_hit
    before = (
        lax.broadcasted_iota(jnp.int32, (count, count), 0)
        < lax.broadcasted_iota(jnp.int32, (count, count), 1)
    )
    position = jnp.dot(
        hit.astype(jnp.float32).astype(jnp.bfloat16),
        before.astype(jnp.float32).astype(jnp.bfloat16),
        preferred_element_type=jnp.float32,
    )
    pos[...] = jnp.full(pos.shape, -1.0, jnp.float32)
    pos[:, 0:count] = jnp.where(hit, position, -1.0)
    pl.semaphore_wait(barrier, len(peers))
    for j in range(1, n_up):
        up_copy(0, j).start()
        up_copy(1, j).start()

    def remote(kind, index, src, dst, peer):
        return pltpu.make_async_remote_copy(
            src_ref=src,
            dst_ref=dst,
            send_sem=send_sems.at[kind, index],
            recv_sem=recv_sems.at[kind, index],
            device_id={"ep": peer},
            device_id_type=MESH,
        )

    chunks = features // CHUNK

    def span(k):
        return pl.ds(k * CHUNK, CHUNK)

    def dense(d, k, src, peer):
        return remote(
            0, d * chunks + k, src.at[:, span(k)], line.at[d - 1, :, span(k)], peer
        )

    def slots(d, src, peer):
        return remote(1, d, src, line_pos.at[d - 1], peer)

    def end_dense(k):
        return dense(1, k, tokens, z_peers[1])

    def mid_dense(k):
        return dense(3, k, tokens, z_peers[3])

    def fwd_dense(k):
        return dense(2, k, line.at[0], z_peers[3])

    end_slots = slots(1, pos, z_peers[1])
    mid_slots = slots(3, pos, z_peers[3])
    fwd_slots = slots(2, line_pos.at[0], z_peers[3])

    def box(p, k):
        return remote(
            2,
            p * chunks + k,
            outbox.at[p - 1, :, span(k)],
            arrived.at[p, 0, :, span(k)],
            z_peers[1],
        )

    def within(kind, p, k, source, target, peer):
        return remote(
            kind,
            p * chunks + k,
            arrived.at[p, source, :, span(k)],
            arrived.at[p, target, :, span(k)],
            peer,
        )

    def y_out(p, k):
        return within(3, p, k, 0, 1, y_peer)

    def c_out(p, k):
        return within(4, p, k, 0, 2, core_peer)

    def f_out(p, k):
        return within(5, p, k, 1, 3, core_peer)

    def c_back(p, j):
        return remote(
            6, p * n_down + j, partial.at[p, j, pl.ds(2, 2)], got_core.at[p, j], core_peer
        )

    def y_back(p, j):
        return remote(7, p * n_down + j, partial.at[p, j, 1], got_y.at[p, j], y_peer)

    def z_back(p, d, j, peer):
        return remote(8, d * n_down + j, partial.at[p, j, 0], got_z.at[d, j], peer)

    def pack(dst, slot, src, k):
        cap = dst.shape[0]
        wanted = lax.broadcasted_iota(jnp.int32, (cap, count), 0).astype(jnp.float32)
        pick = jnp.where(wanted == slot[:, 0:count], 1.0, 0.0).astype(jnp.bfloat16)
        dst[:, span(k)] = jnp.dot(
            pick, src[:, span(k)], preferred_element_type=jnp.float32
        ).astype(jnp.bfloat16)

    def spread(p, k):
        y_out(p, k).start()
        c_out(p, k).start()

    def forward(p, k):
        y_out(p, k).wait_recv()
        f_out(p, k).start()

    def settle(p):
        for k in range(chunks):
            c_out(p, k).wait_recv()
            f_out(p, k).wait_recv()

    @on_end
    def _():
        end_slots.start()
        for k in range(chunks):
            end_dense(k).start()

    @on_mid
    def _():
        mid_slots.start()
        for k in range(chunks):
            mid_dense(k).start()

    for k in range(chunks):
        pack(arrived.at[0, 0], pos[0:1, :], tokens, k)
        spread(0, k)

    @on_mid
    def _():
        for k in range(chunks):
            pack(outbox.at[2], pos[1:2, :], tokens, k)
            box(3, k).start()

    logits = lax.dot_general(
        router[...], tokens[...], (((1,), (1,)), ((), ())), preferred_element_type=jnp.float32
    )
    natural = lax.broadcasted_iota(jnp.int32, (experts, count), 0)
    first = jnp.sum(jnp.where(ids[0:1, :] == natural, logits, 0.0), axis=0, keepdims=True)
    second = jnp.sum(jnp.where(ids[1:2, :] == natural, logits, 0.0), axis=0, keepdims=True)
    first_gate = 1.0 / (1.0 + jnp.exp(second - first))
    second_gate = 1.0 / (1.0 + jnp.exp(first - second))
    gate[...] = jnp.zeros(gate.shape, jnp.float32)
    gate[:, 0:count] = jnp.where(first_hit, first_gate, 0.0) + jnp.where(
        second_hit, second_gate, 0.0
    )
    lanes = pos.shape[1]
    columns = jnp.concatenate(
        [pos[...], gate[...], jnp.zeros((lanes - 16, lanes), jnp.float32)], axis=0
    ).T
    width = experts * CAP
    slot = lax.broadcasted_iota(jnp.int32, (count, width), 1)
    weight = jnp.zeros((count, width), jnp.float32)
    for d in range(experts):
        inside = slot.astype(jnp.float32) == columns[0:count, d : d + 1] + float(d * CAP)
        inside = inside & (columns[0:count, d : d + 1] >= 0.0)
        weight = jnp.where(inside, columns[0:count, 8 + d : 9 + d], weight)
    high = weight.astype(jnp.bfloat16)
    comb[0] = high
    comb[1] = (weight - high.astype(jnp.float32)).astype(jnp.bfloat16)

    kv_copy(0).wait()
    kv_copy(1).wait()
    heads, head_dim = queries.shape[1], queries.shape[2]
    rows = keys.shape[1]

    def attend(r, carry):
        scores = lax.dot_general(
            queries[r], keys[r], (((1,), (1,)), ((), ())), preferred_element_type=jnp.float32
        ) * head_dim ** (-0.5)
        col = lax.broadcasted_iota(jnp.int32, (heads, rows), 1)
        head = lax.broadcasted_iota(jnp.int32, (heads, rows), 0)
        keep = (col % kv_heads == head // (heads // kv_heads)) & (
            col // kv_heads < lengths[r]
        )
        scores = jnp.where(keep, scores, -jnp.inf)
        top = jnp.max(scores, axis=1, keepdims=True)
        expo = jnp.exp(scores - top)
        weights = (expo / jnp.sum(expo, axis=1, keepdims=True)).astype(jnp.bfloat16)
        mixed = jnp.dot(weights, values[r], preferred_element_type=jnp.float32)
        att_out[r] = mixed.astype(att_out.dtype)
        return carry

    lax.fori_loop(0, queries.shape[0], attend, 0)
    for j in range(n_down):
        down_copy(j).start()

    def attend_to(services, j):
        for at, want, action in services:
            pl.when((j == at) if want is None else (j == at) & (mid == want))(action)

    def gate_up(p, wait, services=()):
        block = arrived.at[p]
        m = block.shape[0] * block.shape[1]

        def step(j, carry):
            if wait:
                up_copy(0, j).wait()
                up_copy(1, j).wait()
            x = block[...].reshape(m, features)
            g = jnp.dot(x, wg[j], preferred_element_type=jnp.float32)
            u = jnp.dot(x, wu[j], preferred_element_type=jnp.float32)
            hidden[j] = (g / (1.0 + jnp.exp(-g)) * u).astype(jnp.bfloat16)
            attend_to(services, j)
            return carry

        lax.fori_loop(0, n_up, step, 0)

    def down(p, wait, services=()):
        def step(j, carry):
            if wait:
                down_copy(j).wait()
            h = jnp.concatenate([hidden[i] for i in range(n_up)], axis=1)
            o = jnp.dot(h, wd[j], preferred_element_type=jnp.float32)
            partial[p, j] = o.astype(jnp.bfloat16).reshape(partial.shape[2:])
            c_back(p, j).start()
            attend_to(services, j)
            return carry

        lax.fori_loop(0, n_down, step, 0)

    def sum_core(p, j):
        def action():
            c_back(p, j).wait_recv()
            for s in (1, 0):
                partial[p, j, s] = (
                    partial[p, j, s].astype(jnp.float32) + got_core[p, j, s].astype(jnp.float32)
                ).astype(jnp.bfloat16)
            y_back(p, j).start()

        return action

    def sum_y(p, j):
        def action():
            y_back(p, j).wait_recv()
            total = partial[p, j, 0].astype(jnp.float32) + got_y[p, j].astype(jnp.float32)
            if p == 0:
                got_z[0, j] = total.astype(jnp.bfloat16)
            else:
                partial[p, j, 0] = total.astype(jnp.bfloat16)
                z_back(p, xors[p], j, homes[p]).start()

        return action

    def take(p, k):
        def action():
            box(p, k).wait_recv()
            spread(p, k)

        return action

    def near(k):
        def action():
            end_dense(k).wait_recv()
            fwd_dense(k).start()
            mid_dense(k).wait_recv()
            pack(arrived.at[1, 0], line_pos[2, 3:4, :], line.at[2], k)
            spread(1, k)
            pack(outbox.at[0], line_pos[2, 2:3, :], line.at[2], k)
            box(1, k).start()
            pack(arrived.at[3, 0], line_pos[0, 1:2, :], line.at[0], k)
            spread(3, k)

        return action

    def far(k):
        def action():
            if k == 0:
                fwd_slots.wait_recv()
            fwd_dense(k).wait_recv()
            pack(outbox.at[1], line_pos[1, 3:4, :], line.at[1], k)
            box(2, k).start()
            pack(arrived.at[2, 0], line_pos[1, 2:3, :], line.at[1], k)
            spread(2, k)

        return action

    def forwards(p):
        for k in range(chunks):
            forward(p, k)

    @on_end
    def _():
        for k in range(chunks):
            forward(0, k)
            take(3, k)()

    @on_mid
    def _():
        end_slots.wait_recv()
        fwd_slots.start()
        mid_slots.wait_recv()
        for k in range(chunks - 1):
            forward(0, k)
            near(k)()
        forward(0, chunks - 1)

    settle(0)
    gate_up(
        0,
        True,
        [
            (1, 1, near(chunks - 1)),
            (2, 0, take(1, 0)),
            (3, 0, take(1, 1)),
            (3, 1, far(0)),
        ],
    )
    down(0, True, [(1, 1, far(1)), (1, 0, take(1, 2))])
    forwards(1)
    settle(1)
    gate_up(
        1,
        False,
        [(0, 1, far(2)), (0, 0, take(2, 0)), (1, 0, take(2, 1)), (3, 0, take(2, 2))],
    )
    forwards(3)
    down(1, False, [(1, None, sum_core(1, 0)), (2, None, sum_core(1, 1))])
    forwards(2)
    sum_core(1, 2)()
    sum_core(0, 0)()
    settle(2)
    gate_up(2, False, [(3, None, sum_y(1, 0))])
    down(
        2,
        False,
        [
            (1, None, sum_core(2, 0)),
            (1, None, sum_y(1, 1)),
            (2, None, sum_core(2, 1)),
            (2, None, sum_y(1, 2)),
        ],
    )
    sum_core(2, 2)()
    sum_core(0, 1)()
    settle(3)
    gate_up(3, False, [(3, None, sum_y(2, 0))])
    down(
        3,
        False,
        [
            (1, None, sum_core(3, 0)),
            (1, None, sum_y(2, 1)),
            (2, None, sum_core(3, 1)),
            (2, None, sum_y(2, 2)),
        ],
    )
    sum_core(3, 2)()
    sum_core(0, 2)()
    for j in range(n_down):
        sum_y(3, j)()
    for j in range(n_down):
        sum_y(0, j)()
    for j in range(n_down):
        for d in range(1, experts):
            z_back(d, d, j, z_peers[d]).wait_recv()
        returned = got_z[:, j].reshape(experts * got_z.shape[2], down_tile)
        out[:, j * down_tile : (j + 1) * down_tile] = (
            jnp.dot(comb[0], returned, preferred_element_type=jnp.float32)
            + jnp.dot(comb[1], returned, preferred_element_type=jnp.float32)
        ).astype(out.dtype)

    @on_end
    def _():
        end_slots.wait_send()
        for k in range(chunks):
            end_dense(k).wait_send()

    @on_mid
    def _():
        mid_slots.wait_send()
        fwd_slots.wait_send()
        for k in range(chunks):
            mid_dense(k).wait_send()
            fwd_dense(k).wait_send()
            for p in range(1, experts):
                box(p, k).wait_send()

    for p in range(experts):
        for k in range(chunks):
            y_out(p, k).wait_send()
            c_out(p, k).wait_send()
            f_out(p, k).wait_send()
        for j in range(n_down):
            c_back(p, j).wait_send()
            y_back(p, j).wait_send()
            if p > 0:
                z_back(p, p, j, z_peers[p]).wait_send()


def fused(
    plane,
    tokens,
    expert_ids,
    w_router,
    w_gate,
    w_up,
    w_down,
    queries,
    key_cache,
    cached_value_rows,
    lengths,
):
    experts = w_router.shape[1]
    count, features = tokens.shape
    width = w_gate.shape[1]
    requests, positions, kv_heads, head_dim = key_cache.shape
    flat = (requests, positions * kv_heads, head_dim)
    bf16 = jnp.bfloat16
    f32 = jnp.float32
    lanes = 128
    vmem = pl.BlockSpec(memory_space=pltpu.VMEM)
    smem = pl.BlockSpec(memory_space=pltpu.SMEM)
    hbm = pl.BlockSpec(memory_space=pl.ANY)
    n_up = width // UP_TILE
    n_down = features // DOWN_TILE
    return pl.pallas_call(
        functools.partial(moe_kernel, plane, kv_heads),
        out_shape=(
            jax.ShapeDtypeStruct((count, features), bf16),
            jax.ShapeDtypeStruct(queries.shape, bf16),
        ),
        in_specs=[vmem, vmem, vmem, vmem, smem, hbm, hbm, hbm, hbm, hbm],
        out_specs=(vmem, vmem),
        scratch_shapes=[
            pltpu.VMEM((n_up, features, UP_TILE), bf16),
            pltpu.VMEM((n_up, features, UP_TILE), bf16),
            pltpu.VMEM((n_down, width, DOWN_TILE), bf16),
            pltpu.VMEM(flat, bf16),
            pltpu.VMEM(flat, bf16),
            pltpu.VMEM((8, lanes), f32),
            pltpu.VMEM((8, lanes), f32),
            pltpu.VMEM((2, count, experts * CAP), bf16),
            pltpu.VMEM((experts - 1, count, features), bf16),
            pltpu.VMEM((experts - 1, 8, lanes), f32),
            pltpu.VMEM((experts - 1, CAP, features), bf16),
            pltpu.VMEM((experts, plane, CAP, features), bf16),
            pltpu.VMEM((n_up, plane * CAP, UP_TILE), bf16),
            pltpu.VMEM((experts, n_down, plane, CAP, DOWN_TILE), bf16),
            pltpu.VMEM((experts, n_down, 2, CAP, DOWN_TILE), bf16),
            pltpu.VMEM((experts, n_down, CAP, DOWN_TILE), bf16),
            pltpu.VMEM((experts, n_down, CAP, DOWN_TILE), bf16),
            pltpu.SemaphoreType.DMA((2, n_up)),
            pltpu.SemaphoreType.DMA((n_down,)),
            pltpu.SemaphoreType.DMA((2,)),
            pltpu.SemaphoreType.DMA((9, experts * n_down)),
            pltpu.SemaphoreType.DMA((9, experts * n_down)),
        ],
        compiler_params=pltpu.CompilerParams(
            collective_id=0, has_side_effects=True, vmem_limit_bytes=VMEM_LIMIT
        ),
    )(
        tokens,
        expert_ids.T,
        w_router.T,
        queries,
        lengths,
        w_gate,
        w_up,
        w_down,
        key_cache.reshape(flat),
        cached_value_rows.reshape(flat),
    )


def general(
    share,
    tokens,
    expert_ids,
    w_router,
    w_gate,
    w_up,
    w_down,
    queries,
    key_cache,
    cached_value_rows,
    lengths,
):
    f32 = jnp.float32
    experts = w_router.shape[1]
    logits = jnp.dot(tokens, w_router, preferred_element_type=f32)
    onehot = expert_ids[:, :, None] == jnp.arange(experts, dtype=jnp.int32)[None, None, :]
    picked = jnp.sum(jnp.where(onehot, logits[:, None, :], 0.0), axis=2)
    gates = 1.0 / (1.0 + jnp.exp(picked[:, ::-1] - picked))
    gate_of = jnp.sum(jnp.where(onehot, gates[:, :, None], 0.0), axis=1)
    everyone = lax.all_gather(tokens, "ep", tiled=True)
    gate_of = lax.all_gather(gate_of, "ep", tiled=True)
    mine = jnp.arange(experts, dtype=jnp.int32) == lax.axis_index("ep") // share
    weight = jnp.sum(jnp.where(mine[None, :], gate_of, 0.0), axis=1, keepdims=True)
    g = jnp.dot(everyone, w_gate, preferred_element_type=f32)
    u = jnp.dot(everyone, w_up, preferred_element_type=f32)
    hidden = (g / (1.0 + jnp.exp(-g)) * u).astype(jnp.bfloat16)
    part = jnp.dot(hidden, w_down, preferred_element_type=f32) * weight
    moe_out = lax.psum_scatter(part, "ep", scatter_dimension=0, tiled=True).astype(jnp.bfloat16)
    requests, heads, head_dim = queries.shape
    positions, kv_heads = key_cache.shape[1:3]
    grouped = queries.reshape(requests, kv_heads, heads // kv_heads, head_dim)
    scores = jnp.einsum(
        "bkgd,blkd->bkgl", grouped, key_cache, preferred_element_type=f32
    ) * head_dim ** (-0.5)
    visible = jnp.arange(positions, dtype=jnp.int32)[None, :] < lengths[:, None]
    weights = jax.nn.softmax(jnp.where(visible[:, None, None, :], scores, -jnp.inf), axis=3)
    mixed = jnp.einsum(
        "bkgl,blkd->bkgd",
        weights.astype(jnp.bfloat16),
        cached_value_rows,
        preferred_element_type=f32,
    )
    return moe_out, mixed.reshape(queries.shape).astype(jnp.bfloat16)


def on_device(*args):
    experts = args[2].shape[1]
    share = lax.axis_size("ep") // experts
    body = fused if experts == 4 and share == 4 else general
    return body(share, *args)


def solution(mesh):
    in_specs = (
        P(("group", "ep"), None),
        P(("group", "ep"), None),
        P(),
        P(None, "ep"),
        P(None, "ep"),
        P("ep", None),
        P(("group", "ep"), None, None),
        P(("group", "ep"), None, None, None),
        P(("group", "ep"), None, None, None),
        P(("group", "ep")),
    )
    out_specs = (P(("group", "ep"), None), P(("group", "ep"), None, None))
    return jax.shard_map(
        on_device, mesh=mesh, in_specs=in_specs, out_specs=out_specs, check_vma=False
    )
```

```python
import functools

import jax
import jax.numpy as jnp
from jax import lax
from jax.experimental import pallas as pl
from jax.experimental.pallas import tpu as pltpu
from jax.sharding import PartitionSpec as P

CAP = 48
UP_TILE = 512
DOWN_TILE = 1024
CHUNK = 1024
VMEM_LIMIT = 66_000_000
MESH = pl.DeviceIdType.MESH


def flip(index, mask):
    result = index
    bit = 1
    while bit <= mask:
        if mask & bit:
            result = result + bit - 2 * bit * ((index // bit) % 2)
        bit *= 2
    return result


def moe_kernel(
    plane,
    kv_heads,
    tokens,
    ids,
    router,
    queries,
    lengths,
    wg_hbm,
    wu_hbm,
    wd_hbm,
    k_hbm,
    v_hbm,
    out,
    att_out,
    wg,
    wu,
    wd,
    keys,
    values,
    pos,
    gate,
    comb,
    line,
    line_pos,
    outbox,
    arrived,
    hidden,
    partial,
    got_core,
    got_y,
    got_z,
    w_sems,
    d_sems,
    kv_sems,
    send_sems,
    recv_sems,
):
    me = lax.axis_index("ep")
    experts = router.shape[0]
    count, features = tokens.shape
    z = me // plane
    mid = (z % (experts - 1) + 1) // 2
    core_peer = flip(me, 1)
    y_peer = flip(me, 2)
    z_peers = [flip(me, plane * d) for d in range(experts)]
    xors = [0, 2 + mid, 3 - mid, 1]
    homes = [
        me,
        z_peers[2] + mid * (z_peers[3] - z_peers[2]),
        z_peers[3] + mid * (z_peers[2] - z_peers[3]),
        z_peers[1],
    ]
    n_up = wg.shape[0]
    n_down = wd.shape[0]
    up_tile = wg.shape[2]
    down_tile = wd.shape[2]

    def on_end(body):
        pl.when(mid == 0)(body)

    def on_mid(body):
        pl.when(mid == 1)(body)

    def kv_copy(i):
        src, dst = ((k_hbm, keys), (v_hbm, values))[i]
        return pltpu.make_async_copy(src, dst, kv_sems.at[i])

    def up_copy(i, j):
        src, dst = ((wg_hbm, wg), (wu_hbm, wu))[i]
        cols = pl.ds(pl.multiple_of(j * up_tile, up_tile), up_tile)
        return pltpu.make_async_copy(src.at[:, cols], dst.at[j], w_sems.at[i, j])

    def down_copy(j):
        cols = pl.ds(pl.multiple_of(j * down_tile, down_tile), down_tile)
        return pltpu.make_async_copy(wd_hbm.at[:, cols], wd.at[j], d_sems.at[j])

    barrier = pltpu.get_barrier_semaphore()
    peers = [core_peer, y_peer] + z_peers[1:]
    for peer in peers:
        pl.semaphore_signal(barrier, inc=1, device_id={"ep": peer}, device_id_type=MESH)
    kv_copy(0).start()
    kv_copy(1).start()
    up_copy(0, 0).start()
    up_copy(1, 0).start()

    row = lax.broadcasted_iota(jnp.int32, (8, count), 0)
    label = jnp.full((8, count), -1, jnp.int32)
    for d in range(experts):
        label = jnp.where(row == d, flip(z, d), label)
    first_hit = ids[0:1, :] == label
    second_hit = ids[1:2, :] == label
    hit = first_hit | second_hit
    before = (
        lax.broadcasted_iota(jnp.int32, (count, count), 0)
        < lax.broadcasted_iota(jnp.int32, (count, count), 1)
    )
    position = jnp.dot(
        hit.astype(jnp.float32).astype(jnp.bfloat16),
        before.astype(jnp.float32).astype(jnp.bfloat16),
        preferred_element_type=jnp.float32,
    )
    pos[...] = jnp.full(pos.shape, -1.0, jnp.float32)
    pos[:, 0:count] = jnp.where(hit, position, -1.0)
    pl.semaphore_wait(barrier, len(peers))
    for j in range(1, n_up):
        up_copy(0, j).start()
        up_copy(1, j).start()

    def remote(kind, index, src, dst, peer):
        return pltpu.make_async_remote_copy(
            src_ref=src,
            dst_ref=dst,
            send_sem=send_sems.at[kind, index],
            recv_sem=recv_sems.at[kind, index],
            device_id={"ep": peer},
            device_id_type=MESH,
        )

    chunks = features // CHUNK

    def span(k):
        return pl.ds(k * CHUNK, CHUNK)

    def dense(d, k, src, peer):
        return remote(
            0, d * chunks + k, src.at[:, span(k)], line.at[d - 1, :, span(k)], peer
        )

    def slots(d, src, peer):
        return remote(1, d, src, line_pos.at[d - 1], peer)

    def end_dense(k):
        return dense(1, k, tokens, z_peers[1])

    def mid_dense(k):
        return dense(3, k, tokens, z_peers[3])

    def fwd_dense(k):
        return dense(2, k, line.at[0], z_peers[3])

    end_slots = slots(1, pos, z_peers[1])
    mid_slots = slots(3, pos, z_peers[3])
    fwd_slots = slots(2, line_pos.at[0], z_peers[3])

    def box(p, k):
        return remote(
            2,
            p * chunks + k,
            outbox.at[p - 1, :, span(k)],
            arrived.at[p, 0, :, span(k)],
            z_peers[1],
        )

    def within(kind, p, k, source, target, peer):
        return remote(
            kind,
            p * chunks + k,
            arrived.at[p, source, :, span(k)],
            arrived.at[p, target, :, span(k)],
            peer,
        )

    def y_out(p, k):
        return within(3, p, k, 0, 1, y_peer)

    def c_out(p, k):
        return within(4, p, k, 0, 2, core_peer)

    def f_out(p, k):
        return within(5, p, k, 1, 3, core_peer)

    def c_back(p, j):
        return remote(
            6, p * n_down + j, partial.at[p, j, pl.ds(2, 2)], got_core.at[p, j], core_peer
        )

    def y_back(p, j):
        return remote(7, p * n_down + j, partial.at[p, j, 1], got_y.at[p, j], y_peer)

    def z_back(p, d, j, peer):
        return remote(8, d * n_down + j, partial.at[p, j, 0], got_z.at[d, j], peer)

    def pack(dst, slot, src, k):
        cap = dst.shape[0]
        wanted = lax.broadcasted_iota(jnp.int32, (cap, count), 0).astype(jnp.float32)
        pick = jnp.where(wanted == slot[:, 0:count], 1.0, 0.0).astype(jnp.bfloat16)
        dst[:, span(k)] = jnp.dot(
            pick, src[:, span(k)], preferred_element_type=jnp.float32
        ).astype(jnp.bfloat16)

    def spread(p, k):
        y_out(p, k).start()
        c_out(p, k).start()

    def forward(p, k):
        y_out(p, k).wait_recv()
        f_out(p, k).start()

    def settle(p):
        for k in range(chunks):
            c_out(p, k).wait_recv()
            f_out(p, k).wait_recv()

    @on_end
    def _():
        end_slots.start()
        for k in range(chunks):
            end_dense(k).start()

    @on_mid
    def _():
        mid_slots.start()
        for k in range(chunks):
            mid_dense(k).start()

    for k in range(chunks):
        pack(arrived.at[0, 0], pos[0:1, :], tokens, k)
        spread(0, k)

    @on_mid
    def _():
        for k in range(chunks):
            pack(outbox.at[2], pos[1:2, :], tokens, k)
            box(3, k).start()

    logits = lax.dot_general(
        router[...], tokens[...], (((1,), (1,)), ((), ())), preferred_element_type=jnp.float32
    )
    natural = lax.broadcasted_iota(jnp.int32, (experts, count), 0)
    first = jnp.sum(jnp.where(ids[0:1, :] == natural, logits, 0.0), axis=0, keepdims=True)
    second = jnp.sum(jnp.where(ids[1:2, :] == natural, logits, 0.0), axis=0, keepdims=True)
    first_gate = 1.0 / (1.0 + jnp.exp(second - first))
    second_gate = 1.0 / (1.0 + jnp.exp(first - second))
    gate[...] = jnp.zeros(gate.shape, jnp.float32)
    gate[:, 0:count] = jnp.where(first_hit, first_gate, 0.0) + jnp.where(
        second_hit, second_gate, 0.0
    )
    lanes = pos.shape[1]
    columns = jnp.concatenate(
        [pos[...], gate[...], jnp.zeros((lanes - 16, lanes), jnp.float32)], axis=0
    ).T
    width = experts * CAP
    slot = lax.broadcasted_iota(jnp.int32, (count, width), 1)
    weight = jnp.zeros((count, width), jnp.float32)
    for d in range(experts):
        inside = slot.astype(jnp.float32) == columns[0:count, d : d + 1] + float(d * CAP)
        inside = inside & (columns[0:count, d : d + 1] >= 0.0)
        weight = jnp.where(inside, columns[0:count, 8 + d : 9 + d], weight)
    high = weight.astype(jnp.bfloat16)
    comb[0] = high
    comb[1] = (weight - high.astype(jnp.float32)).astype(jnp.bfloat16)

    kv_copy(0).wait()
    kv_copy(1).wait()
    heads, head_dim = queries.shape[1], queries.shape[2]
    rows = keys.shape[1]

    def attend(r, carry):
        scores = lax.dot_general(
            queries[r], keys[r], (((1,), (1,)), ((), ())), preferred_element_type=jnp.float32
        ) * head_dim ** (-0.5)
        col = lax.broadcasted_iota(jnp.int32, (heads, rows), 1)
        head = lax.broadcasted_iota(jnp.int32, (heads, rows), 0)
        keep = (col % kv_heads == head // (heads // kv_heads)) & (
            col // kv_heads < lengths[r]
        )
        scores = jnp.where(keep, scores, -jnp.inf)
        top = jnp.max(scores, axis=1, keepdims=True)
        expo = jnp.exp(scores - top)
        weights = (expo / jnp.sum(expo, axis=1, keepdims=True)).astype(jnp.bfloat16)
        mixed = jnp.dot(weights, values[r], preferred_element_type=jnp.float32)
        att_out[r] = mixed.astype(att_out.dtype)
        return carry

    lax.fori_loop(0, queries.shape[0], attend, 0)
    for j in range(n_down):
        down_copy(j).start()

    def attend_to(services, j):
        for at, want, action in services:
            pl.when((j == at) if want is None else (j == at) & (mid == want))(action)

    def gate_up(p, wait, services=()):
        block = arrived.at[p]
        m = block.shape[0] * block.shape[1]

        def step(j, carry):
            if wait:
                up_copy(0, j).wait()
                up_copy(1, j).wait()
            x = block[...].reshape(m, features)
            g = jnp.dot(x, wg[j], preferred_element_type=jnp.float32)
            u = jnp.dot(x, wu[j], preferred_element_type=jnp.float32)
            hidden[j] = (g / (1.0 + jnp.exp(-g)) * u).astype(jnp.bfloat16)
            attend_to(services, j)
            return carry

        lax.fori_loop(0, n_up, step, 0)

    def down(p, wait, services=()):
        def step(j, carry):
            if wait:
                down_copy(j).wait()
            h = jnp.concatenate([hidden[i] for i in range(n_up)], axis=1)
            o = jnp.dot(h, wd[j], preferred_element_type=jnp.float32)
            partial[p, j] = o.astype(jnp.bfloat16).reshape(partial.shape[2:])
            c_back(p, j).start()
            attend_to(services, j)
            return carry

        lax.fori_loop(0, n_down, step, 0)

    def sum_core(p, j):
        def action():
            c_back(p, j).wait_recv()
            for s in (1, 0):
                partial[p, j, s] = (
                    partial[p, j, s].astype(jnp.float32) + got_core[p, j, s].astype(jnp.float32)
                ).astype(jnp.bfloat16)
            y_back(p, j).start()

        return action

    def sum_y(p, j):
        def action():
            y_back(p, j).wait_recv()
            total = partial[p, j, 0].astype(jnp.float32) + got_y[p, j].astype(jnp.float32)
            if p == 0:
                got_z[0, j] = total.astype(jnp.bfloat16)
            else:
                partial[p, j, 0] = total.astype(jnp.bfloat16)
                z_back(p, xors[p], j, homes[p]).start()

        return action

    def take(p, k):
        def action():
            box(p, k).wait_recv()
            spread(p, k)

        return action

    def near(k):
        def action():
            end_dense(k).wait_recv()
            fwd_dense(k).start()
            mid_dense(k).wait_recv()
            pack(arrived.at[1, 0], line_pos[2, 3:4, :], line.at[2], k)
            spread(1, k)
            pack(outbox.at[0], line_pos[2, 2:3, :], line.at[2], k)
            box(1, k).start()
            pack(arrived.at[3, 0], line_pos[0, 1:2, :], line.at[0], k)
            spread(3, k)

        return action

    def far(k):
        def action():
            if k == 0:
                fwd_slots.wait_recv()
            fwd_dense(k).wait_recv()
            pack(outbox.at[1], line_pos[1, 3:4, :], line.at[1], k)
            box(2, k).start()
            pack(arrived.at[2, 0], line_pos[1, 2:3, :], line.at[1], k)
            spread(2, k)

        return action

    def pass_on(p, k):
        return lambda: forward(p, k)

    def forwards(p):
        for k in range(chunks):
            forward(p, k)

    @on_end
    def _():
        for k in range(chunks):
            forward(0, k)
            take(3, k)()

    @on_mid
    def _():
        end_slots.wait_recv()
        fwd_slots.start()
        mid_slots.wait_recv()
        for k in range(chunks - 1):
            forward(0, k)
            near(k)()
        forward(0, chunks - 1)

    settle(0)
    gate_up(
        0,
        True,
        [
            (1, 1, near(chunks - 1)),
            (2, 0, take(1, 0)),
            (3, 0, take(1, 1)),
            (3, 1, far(0)),
            (3, None, pass_on(1, 0)),
        ],
    )
    down(
        0,
        True,
        [
            (0, 0, take(1, 2)),
            (0, None, pass_on(1, 1)),
            (1, 1, far(1)),
            (1, None, pass_on(1, 2)),
        ],
    )
    settle(1)
    gate_up(
        1,
        False,
        [(0, 1, far(2)), (0, 0, take(2, 0)), (1, 0, take(2, 1)), (3, 0, take(2, 2))],
    )
    forwards(3)
    down(
        1,
        False,
        [
            (0, None, pass_on(2, 0)),
            (1, None, sum_core(1, 0)),
            (1, None, pass_on(2, 1)),
            (2, None, sum_core(1, 1)),
            (2, None, pass_on(2, 2)),
        ],
    )
    settle(2)
    gate_up(
        2,
        False,
        [(0, None, sum_core(1, 2)), (0, None, sum_core(0, 0)), (3, None, sum_y(1, 0))],
    )
    down(
        2,
        False,
        [
            (1, None, sum_core(2, 0)),
            (1, None, sum_y(1, 1)),
            (2, None, sum_core(2, 1)),
            (2, None, sum_y(1, 2)),
        ],
    )
    settle(3)
    gate_up(
        3,
        False,
        [(0, None, sum_core(2, 2)), (0, None, sum_core(0, 1))],
    )
    down(
        3,
        False,
        [
            (1, None, sum_core(3, 0)),
            (1, None, sum_y(2, 0)),
            (2, None, sum_core(3, 1)),
            (2, None, sum_y(2, 1)),
        ],
    )
    sum_core(3, 2)()
    sum_y(2, 2)()
    sum_core(0, 2)()
    for j in range(n_down):
        sum_y(3, j)()
    for j in range(n_down):
        sum_y(0, j)()
    for j in range(n_down):
        for d in range(1, experts):
            z_back(d, d, j, z_peers[d]).wait_recv()
        returned = got_z[:, j].reshape(experts * got_z.shape[2], down_tile)
        out[:, j * down_tile : (j + 1) * down_tile] = (
            jnp.dot(comb[0], returned, preferred_element_type=jnp.float32)
            + jnp.dot(comb[1], returned, preferred_element_type=jnp.float32)
        ).astype(out.dtype)

    @on_end
    def _():
        end_slots.wait_send()
        for k in range(chunks):
            end_dense(k).wait_send()

    @on_mid
    def _():
        mid_slots.wait_send()
        fwd_slots.wait_send()
        for k in range(chunks):
            mid_dense(k).wait_send()
            fwd_dense(k).wait_send()
            for p in range(1, experts):
                box(p, k).wait_send()

    for p in range(experts):
        for k in range(chunks):
            y_out(p, k).wait_send()
            c_out(p, k).wait_send()
            f_out(p, k).wait_send()
        for j in range(n_down):
            c_back(p, j).wait_send()
            y_back(p, j).wait_send()
            if p > 0:
                z_back(p, p, j, z_peers[p]).wait_send()


def fused(
    plane,
    tokens,
    expert_ids,
    w_router,
    w_gate,
    w_up,
    w_down,
    queries,
    key_cache,
    cached_value_rows,
    lengths,
):
    experts = w_router.shape[1]
    count, features = tokens.shape
    width = w_gate.shape[1]
    requests, positions, kv_heads, head_dim = key_cache.shape
    flat = (requests, positions * kv_heads, head_dim)
    bf16 = jnp.bfloat16
    f32 = jnp.float32
    lanes = 128
    vmem = pl.BlockSpec(memory_space=pltpu.VMEM)
    smem = pl.BlockSpec(memory_space=pltpu.SMEM)
    hbm = pl.BlockSpec(memory_space=pl.ANY)
    n_up = width // UP_TILE
    n_down = features // DOWN_TILE
    return pl.pallas_call(
        functools.partial(moe_kernel, plane, kv_heads),
        out_shape=(
            jax.ShapeDtypeStruct((count, features), bf16),
            jax.ShapeDtypeStruct(queries.shape, bf16),
        ),
        in_specs=[vmem, vmem, vmem, vmem, smem, hbm, hbm, hbm, hbm, hbm],
        out_specs=(vmem, vmem),
        scratch_shapes=[
            pltpu.VMEM((n_up, features, UP_TILE), bf16),
            pltpu.VMEM((n_up, features, UP_TILE), bf16),
            pltpu.VMEM((n_down, width, DOWN_TILE), bf16),
            pltpu.VMEM(flat, bf16),
            pltpu.VMEM(flat, bf16),
            pltpu.VMEM((8, lanes), f32),
            pltpu.VMEM((8, lanes), f32),
            pltpu.VMEM((2, count, experts * CAP), bf16),
            pltpu.VMEM((experts - 1, count, features), bf16),
            pltpu.VMEM((experts - 1, 8, lanes), f32),
            pltpu.VMEM((experts - 1, CAP, features), bf16),
            pltpu.VMEM((experts, plane, CAP, features), bf16),
            pltpu.VMEM((n_up, plane * CAP, UP_TILE), bf16),
            pltpu.VMEM((experts, n_down, plane, CAP, DOWN_TILE), bf16),
            pltpu.VMEM((experts, n_down, 2, CAP, DOWN_TILE), bf16),
            pltpu.VMEM((experts, n_down, CAP, DOWN_TILE), bf16),
            pltpu.VMEM((experts, n_down, CAP, DOWN_TILE), bf16),
            pltpu.SemaphoreType.DMA((2, n_up)),
            pltpu.SemaphoreType.DMA((n_down,)),
            pltpu.SemaphoreType.DMA((2,)),
            pltpu.SemaphoreType.DMA((9, experts * n_down)),
            pltpu.SemaphoreType.DMA((9, experts * n_down)),
        ],
        compiler_params=pltpu.CompilerParams(
            collective_id=0, has_side_effects=True, vmem_limit_bytes=VMEM_LIMIT
        ),
    )(
        tokens,
        expert_ids.T,
        w_router.T,
        queries,
        lengths,
        w_gate,
        w_up,
        w_down,
        key_cache.reshape(flat),
        cached_value_rows.reshape(flat),
    )


def general(
    share,
    tokens,
    expert_ids,
    w_router,
    w_gate,
    w_up,
    w_down,
    queries,
    key_cache,
    cached_value_rows,
    lengths,
):
    f32 = jnp.float32
    experts = w_router.shape[1]
    logits = jnp.dot(tokens, w_router, preferred_element_type=f32)
    onehot = expert_ids[:, :, None] == jnp.arange(experts, dtype=jnp.int32)[None, None, :]
    picked = jnp.sum(jnp.where(onehot, logits[:, None, :], 0.0), axis=2)
    gates = 1.0 / (1.0 + jnp.exp(picked[:, ::-1] - picked))
    gate_of = jnp.sum(jnp.where(onehot, gates[:, :, None], 0.0), axis=1)
    everyone = lax.all_gather(tokens, "ep", tiled=True)
    gate_of = lax.all_gather(gate_of, "ep", tiled=True)
    mine = jnp.arange(experts, dtype=jnp.int32) == lax.axis_index("ep") // share
    weight = jnp.sum(jnp.where(mine[None, :], gate_of, 0.0), axis=1, keepdims=True)
    g = jnp.dot(everyone, w_gate, preferred_element_type=f32)
    u = jnp.dot(everyone, w_up, preferred_element_type=f32)
    hidden = (g / (1.0 + jnp.exp(-g)) * u).astype(jnp.bfloat16)
    part = jnp.dot(hidden, w_down, preferred_element_type=f32) * weight
    moe_out = lax.psum_scatter(part, "ep", scatter_dimension=0, tiled=True).astype(jnp.bfloat16)
    requests, heads, head_dim = queries.shape
    positions, kv_heads = key_cache.shape[1:3]
    grouped = queries.reshape(requests, kv_heads, heads // kv_heads, head_dim)
    scores = jnp.einsum(
        "bkgd,blkd->bkgl", grouped, key_cache, preferred_element_type=f32
    ) * head_dim ** (-0.5)
    visible = jnp.arange(positions, dtype=jnp.int32)[None, :] < lengths[:, None]
    weights = jax.nn.softmax(jnp.where(visible[:, None, None, :], scores, -jnp.inf), axis=3)
    mixed = jnp.einsum(
        "bkgl,blkd->bkgd",
        weights.astype(jnp.bfloat16),
        cached_value_rows,
        preferred_element_type=f32,
    )
    return moe_out, mixed.reshape(queries.shape).astype(jnp.bfloat16)


def on_device(*args):
    experts = args[2].shape[1]
    share = lax.axis_size("ep") // experts
    body = fused if experts == 4 and share == 4 else general
    return body(share, *args)


def solution(mesh):
    in_specs = (
        P(("group", "ep"), None),
        P(("group", "ep"), None),
        P(),
        P(None, "ep"),
        P(None, "ep"),
        P("ep", None),
        P(("group", "ep"), None, None),
        P(("group", "ep"), None, None, None),
        P(("group", "ep"), None, None, None),
        P(("group", "ep")),
    )
    out_specs = (P(("group", "ep"), None), P(("group", "ep"), None, None))
    return jax.shard_map(
        on_device, mesh=mesh, in_specs=in_specs, out_specs=out_specs, check_vma=False
    )
```
